256 devices in a mesh: dp: 16 (over z_lo, x), shard: 16 (over z_hi, y, core).
Axes of the slice: x: 4, y: 4, z: 8 (z_hi: 2, z_lo: 4; z = z_hi * 4 + z_lo), core: 2. Of those that a mesh axis runs over, the one named last changes fastest.
Arguments:
- hidden_in: bfloat16 [65536, 5120], P(('dp', 'shard')), may hold values from -24 to 24
- teacher: bfloat16 [65536, 768], P(('dp', 'shard')), may hold values from -6 to 6
- norm_gain: bfloat16 [5120], P('shard'), may hold values from 0.5 to 1.5
- w_key: bfloat16 [5120, 768], P('shard'), may hold values from -0.078125 to 0.078125
- group_rows: int32 [16], P('dp'), may hold values from 64 to 256
- member: int32 [16, 16], P('dp', 'shard'), may hold values from 0 to 1, as said below
Outputs:
- loss: float32 [], replicated
- grad_gain: float32 [5120], P('shard')
- grad_key: float32 [5120, 768], P('shard')
The draws below stay inside these ranges and needn't reach their ends.
Inputs may be any that keep to these rules, and one draw needn't show every extreme that they name: The first group_rows[p] token slots of each surviving device of group p hold valid tokens. `member`: 1 marks a surviving device; the first device of every group survives.
All inputs are finite; a program needn't handle non-finite values.
Results may differ from the reference program's by a relative error of at most 0.0023.
Values may be sent and summed in bfloat16 or wider, within the bound.
No kernel may reach another device: no remote copies, remote signals or barrier semaphores. Data moves between devices by JAX's collectives and lax.ppermute only.
A program may use at most 128 MiB of HBM per device.

```python
import jax
import jax.numpy as jnp
from jax import lax

D = 5120
KV = 768
TOK_DEV = 256
GROUPS = 16
MEMBERS = 16
TOKENS = 65536


def draw_member(key, part):
    picks = jax.random.randint(key, (GROUPS, MEMBERS), 0, 4)
    first = jnp.arange(MEMBERS)[None, :] == 0
    return jnp.where((picks > 0) | first, 1, 0).astype(jnp.int32)


def touch_ends(values, key, low, top_value):
    longest = values.shape.index(max(values.shape))
    spots = []
    for shift in (0, 1):
        where = [jax.random.randint(jax.random.fold_in(key, axis), (), 0, length) for axis, length in enumerate(values.shape)]
        where[longest] = (where[longest] + shift) % values.shape[longest]
        spots.append(tuple(where))
    return values.at[spots[0]].set(low).at[spots[1]].set(top_value)


def strengthened(drawn, key, source, target, blocks, factor):
    owner, partner = [(jnp.arange(drawn.shape[dim]) // (drawn.shape[dim] // blocks)).reshape([-1 if axis == dim else 1 for axis in range(drawn.ndim)]) for dim in (source, target)]
    chosen = jax.random.permutation(key, blocks)[partner]
    strong = (owner == chosen) | (owner == (partner + blocks // 2) % blocks)
    return jnp.where(strong, factor * drawn, drawn)


def block_scale(rng, dims, cuts, smallest, high):
    gain, own = 1.0, jax.random.fold_in(rng, 6)
    for dim, shards_of in cuts:
        draws = jnp.exp(jax.random.uniform(jax.random.fold_in(own, dim), (shards_of,), jnp.float32, smallest / len(cuts), high / len(cuts)))
        gain = gain * jnp.repeat(draws, dims[dim] // shards_of).reshape([-1 if axis == dim else 1 for axis in range(len(dims))])
    return gain


def noise(rng, shape, deviation, limit, cuts=(), dtype=jnp.bfloat16):
    result = deviation * jax.random.normal(rng, shape, jnp.float32)
    if cuts:
        result = result * block_scale(rng, shape, cuts, -0.22, 0.18)
    return jnp.clip(result, -limit, limit).astype(dtype)


def noise_with(rng, extent, deviation, limit, pieces, heavy, held_as=jnp.bfloat16):
    values = deviation * jax.random.normal(rng, extent, jnp.float32)
    if pieces:
        values = values * block_scale(rng, extent, pieces, -0.22, 0.18)
    return jnp.clip(strengthened(values, jax.random.fold_in(rng, 3), *heavy), -limit, limit).astype(held_as)


def setup_inputs(seed: int = 0) -> dict:
    seeds = jax.random.split(jax.random.key(seed), 7)
    return {
        "hidden_in": noise_with(seeds[0], (TOKENS, D), 1.0, 24.0, ((0, 256),), (0, 1, 256, 6.0)),
        "teacher": noise(seeds[1], (TOKENS, KV), 1.0, 6.0, ((0, 256),)),
        "norm_gain": jnp.clip(1.0 + 0.1 * jax.random.normal(seeds[2], (D,), jnp.float32), 0.5, 1.5).astype(jnp.bfloat16),
        "w_key": noise(seeds[3], (D, KV), D ** -0.5, 0.078125, ((0, 16),)),
        "group_rows": touch_ends(jax.random.randint(seeds[4], (GROUPS,), TOK_DEV // 4, TOK_DEV + 1), jax.random.fold_in(seeds[4], 1), TOK_DEV // 4, TOK_DEV).astype(jnp.int32),
        "member": draw_member(jax.random.fold_in(seeds[6], 71), 0),
    }


EPSILON = 1e-06
SCALE = 1024.0

def reference(hidden_in, teacher, norm_gain, w_key, group_rows, member):
    blocks = GROUPS * MEMBERS
    live_rows = jnp.repeat(group_rows, MEMBERS).astype(jnp.int32)
    alive = member.reshape(blocks).astype(jnp.int32)
    total_count = jnp.sum(member.astype(jnp.float32) * group_rows.astype(jnp.float32)[:, None])
    gains = norm_gain.astype(jnp.float32)

    def one_block(carry, inputs):
        loss_sum, gain_acc, key_acc = carry
        block_in, block_teacher, block_rows, block_alive = inputs
        position = lax.broadcasted_iota(jnp.int32, (TOK_DEV, 1), 0)
        valid = jnp.where((position < block_rows) & (block_alive == 1), 1.0, 0.0).astype(jnp.float32)
        values = block_in.astype(jnp.float32)
        inverse_rms = lax.rsqrt(lax.optimization_barrier(jnp.mean(values * values, axis=1, keepdims=True)) + EPSILON)
        scaled = values * inverse_rms
        normed = (scaled * gains).astype(jnp.bfloat16)
        keys = jnp.dot(normed, w_key, preferred_element_type=jnp.float32)
        diff = keys - block_teacher.astype(jnp.float32)
        loss_sum = loss_sum + jnp.sum(valid * diff * diff)
        upstream = (SCALE / total_count * valid * diff).astype(jnp.bfloat16)
        term_key = jnp.dot(normed.T, upstream, preferred_element_type=jnp.float32)
        dnormed = jnp.dot(upstream, w_key.T, preferred_element_type=jnp.float32)
        term_gain = lax.optimization_barrier(jnp.sum(dnormed * scaled, axis=0))
        return ((loss_sum, gain_acc + term_gain, key_acc + term_key), None)
    start = (jnp.zeros((), jnp.float32), jnp.zeros((D,), jnp.float32), jnp.zeros((D, KV), jnp.float32))
    inputs = (hidden_in.reshape(blocks, TOK_DEV, D), teacher.reshape(blocks, TOK_DEV, KV), live_rows, alive)
    final, unused = lax.scan(one_block, start, inputs)
    loss_sum, gain_acc, key_acc = final
    loss = loss_sum / (2.0 * KV * total_count)
    return (loss, gain_acc, key_acc)
```

```python
import jax
import jax.numpy as jnp
from jax import lax
from jax.sharding import Mesh
from jax.sharding import PartitionSpec as P

ZL, X, ZH, Y, C = "dp_0", "dp_1", "shard_0", "shard_1", "shard_2"
SHARD = (ZH, Y, C)
DP_SHARD = (ZL, X, ZH, Y, C)
DP = (ZL, X)

EPSILON = 1e-06
SCALE = 1024.0


def fetch(value, axis, step):
    n = lax.axis_size(axis)
    return lax.ppermute(value, axis, [((i + step) % n, i) for i in range(n)])


def ring_blocks(value, axis):
    one, three, two = (fetch(value, axis, step) for step in (1, 3, 2))
    return [value, one, two, three]


def from_everyone(value, axes):
    copies = jnp.broadcast_to(value, (lax.axis_size(axes), *value.shape))
    return lax.all_to_all(copies, axes, split_axis=0, concat_axis=0, tiled=True)


def summed(value, axes):
    tile = jnp.broadcast_to(value, (8, 128))
    return from_everyone(tile, axes)[:, 0, 0].sum()


def rolled(value, start):
    return lax.dynamic_slice_in_dim(jnp.concatenate([value, value]), start, value.shape[0])


def after(value, *others):
    return lax.optimization_barrier((value, *others))[0]


def rows_by(left, right):
    return lax.dot_general(left, right, (((0,), (0,)), ((), ())), preferred_element_type=jnp.float32)


def body(hidden_in, teacher, norm_gain, w_key, group_rows, member):
    rows, width = hidden_in.shape
    own, features = w_key.shape
    part = own // 4
    x, y, zh, core = (lax.axis_index(name) for name in (X, Y, ZH, C))

    other = fetch(lax.dynamic_slice_in_dim(w_key, x * part, part), ZH, 1)
    near = ring_blocks(w_key, Y)
    quarter = jnp.stack(ring_blocks(other, Y))
    far = ring_blocks(quarter, X)

    live_rows = group_rows[0]
    alive = member[0, 0]
    own_count = (alive * live_rows).astype(jnp.float32)
    gain_rows = jnp.pad(norm_gain.astype(jnp.float32), (0, 384 - own)).reshape(3, 128)
    tile = jnp.concatenate([gain_rows, jnp.broadcast_to(own_count, (5, 128))])
    tiles = from_everyone(tile, SHARD)
    gains = tiles[:, :3].reshape(-1, 384)[:, :own].reshape(width)
    total_count = summed(tiles[:, 3, 0].sum(), DP)

    values = hidden_in.astype(jnp.float32)
    inverse_rms = lax.rsqrt(jnp.mean(values * values, axis=1, keepdims=True) + EPSILON)
    normed = (values * inverse_rms * gains).astype(jnp.bfloat16)

    turned = normed.T.reshape(2, 4, 2, own, rows)
    mine = lax.dynamic_index_in_dim(turned, core, 2, keepdims=False)
    theirs = lax.dynamic_index_in_dim(turned, 1 - core, 2, keepdims=False)
    pair = jnp.concatenate([mine, fetch(theirs, C, 1)], axis=-1)
    near_half = rolled(lax.dynamic_index_in_dim(pair, zh, 0, keepdims=False), y)
    far_half = rolled(lax.dynamic_index_in_dim(pair, 1 - zh, 0, keepdims=False), y)
    far_half = far_half.reshape(4, 4, part, 2 * rows).swapaxes(0, 1)
    far_half = rolled(far_half, x)

    halves = sum(rows_by(near_half[i], near[i]) for i in range(4))
    halves += sum(rows_by(far_half[i].reshape(own, -1), far[i].reshape(own, -1)) for i in range(4))
    keys = halves[:rows] + fetch(halves[rows:], C, 1)

    position = lax.broadcasted_iota(jnp.int32, (rows, 1), 0)
    valid = jnp.where((position < live_rows) & (alive == 1), 1.0, 0.0).astype(jnp.float32)
    diff = keys - teacher.astype(jnp.float32)
    own_sum = jnp.sum(valid * diff * diff)
    upstream = (SCALE / total_count * valid * diff).astype(jnp.bfloat16)

    def both_cores(block):
        return jnp.concatenate([block, fetch(block, C, 1)])

    near_in = [near_half[0]] + [fetch(after(near_half[4 - s], near[2]), Y, s) for s in (1, 2, 3)]
    far_in = [far_half[0]] + [fetch(after(far_half[4 - s], far[2]), X, s) for s in (1, 2, 3)]
    near_up = [both_cores(block) for block in ring_blocks(upstream, Y)]
    far_up = [near_up[0]] + [both_cores(block) for block in ring_blocks(upstream, X)[1:]]

    def product(left, right):
        return jnp.dot(left.reshape(own, -1), right, preferred_element_type=jnp.float32)

    near_out = sum(product(a, b) for a, b in zip(near_in, near_up)).reshape(4, part, features)
    far_out = sum(product(a, b) for a, b in zip(far_in, far_up)).reshape(4, part, features)
    near_out = rolled(near_out, x)
    near_sum = near_out[0] + sum(fetch(near_out[4 - s], X, s) for s in (1, 2, 3))
    far_sum = far_out[0] + sum(fetch(far_out[4 - s], Y, s) for s in (1, 2, 3))
    both = jnp.where(zh == 0, jnp.stack([near_sum, far_sum]), jnp.stack([far_sum, near_sum]))

    half, side = part // 2, features // 2
    pieces = both.reshape(2, 2, half, 2, side).transpose(0, 1, 3, 2, 4).reshape(8, half, side)
    piece = lax.all_to_all(pieces, (ZH, ZL), split_axis=0, concat_axis=0, tiled=True).sum(axis=0)
    whole = from_everyone(piece, DP).reshape(2, 2, 4, half, side)
    grad_key = whole.transpose(2, 0, 3, 1, 4).reshape(own, features)
    grad_gain = jnp.sum(w_key.astype(jnp.float32) * grad_key, axis=1) / norm_gain.astype(jnp.float32)

    total_sum = summed(summed(own_sum, SHARD), DP)
    loss = total_sum / (2.0 * features * total_count)
    return (loss, grad_gain, grad_key)


def solution(mesh):
    split = Mesh(mesh.devices.reshape(4, 4, 2, 4, 2), DP_SHARD)
    return jax.shard_map(
        body,
        mesh=split,
        in_specs=(
            P(DP_SHARD, None),
            P(DP_SHARD, None),
            P(SHARD),
            P(SHARD, None),
            P(DP),
            P(DP, SHARD),
        ),
        out_specs=(P(), P(SHARD), P(SHARD, None)),
        check_vma=False,
    )
```

```python
import jax
import jax.numpy as jnp
from jax import lax
from jax.sharding import Mesh
from jax.sharding import PartitionSpec as P

ZL, X, ZH, Y, C = "dp_0", "dp_1", "shard_0", "shard_1", "shard_2"
SHARD = (ZH, Y, C)
DP_SHARD = (ZL, X, ZH, Y, C)
DP = (ZL, X)

EPSILON = 1e-06
SCALE = 1024.0


def fetch(value, axis, step):
    n = lax.axis_size(axis)
    return lax.ppermute(value, axis, [((i + step) % n, i) for i in range(n)])


def ring_blocks(value, axis):
    one, three, two = (fetch(value, axis, step) for step in (1, 3, 2))
    return [value, one, two, three]


def from_everyone(value, axes):
    copies = jnp.broadcast_to(value, (lax.axis_size(axes), *value.shape))
    return lax.all_to_all(copies, axes, split_axis=0, concat_axis=0, tiled=True)


def summed(value, axes):
    tile = jnp.broadcast_to(value, (8, 128))
    return from_everyone(tile, axes)[:, 0, 0].sum()


def rolled(value, start):
    return lax.dynamic_slice_in_dim(jnp.concatenate([value, value]), start, value.shape[0])


def rows_by(left, right):
    return lax.dot_general(left, right, (((0,), (0,)), ((), ())), preferred_element_type=jnp.float32)


def body(hidden_in, teacher, norm_gain, w_key, group_rows, member):
    rows, width = hidden_in.shape
    own, features = w_key.shape
    part = own // 4
    x, y, zh, core = (lax.axis_index(name) for name in (X, Y, ZH, C))

    other = fetch(lax.dynamic_slice_in_dim(w_key, x * part, part), ZH, 1)
    near = ring_blocks(w_key, Y)
    quarter = jnp.stack(ring_blocks(other, Y))
    far = [block.reshape(own, features) for block in ring_blocks(quarter, X)]

    live_rows = group_rows[0]
    alive = member[0, 0]
    own_count = (alive * live_rows).astype(jnp.float32)
    gain_rows = jnp.pad(norm_gain.astype(jnp.float32), (0, 384 - own)).reshape(3, 128)
    tile = jnp.concatenate([gain_rows, jnp.broadcast_to(own_count, (5, 128))])
    tiles = from_everyone(tile, SHARD)
    gains = tiles[:, :3].reshape(-1, 384)[:, :own].reshape(width)
    total_count = summed(tiles[:, 3, 0].sum(), DP)

    values = hidden_in.astype(jnp.float32)
    inverse_rms = lax.rsqrt(jnp.mean(values * values, axis=1, keepdims=True) + EPSILON)
    normed = (values * inverse_rms * gains).astype(jnp.bfloat16)

    turned = normed.T.reshape(2, 4, 2, own, rows)
    mine = lax.dynamic_index_in_dim(turned, core, 2, keepdims=False)
    theirs = lax.dynamic_index_in_dim(turned, 1 - core, 2, keepdims=False)
    pair = jnp.concatenate([mine, fetch(theirs, C, 1)], axis=-1)
    near_half = rolled(lax.dynamic_index_in_dim(pair, zh, 0, keepdims=False), y)
    far_half = rolled(lax.dynamic_index_in_dim(pair, 1 - zh, 0, keepdims=False), y)
    far_half = far_half.reshape(4, 4, part, 2 * rows).swapaxes(0, 1)
    far_half = rolled(far_half, x).reshape(4, own, 2 * rows)

    halves = sum(rows_by(near_half[i], near[i]) for i in range(4)) + rows_by(far_half[0], far[0])
    halves += sum(rows_by(far_half[i], far[i]) for i in (1, 3, 2))
    keys = halves[:rows] + fetch(halves[rows:], C, 1)

    position = lax.broadcasted_iota(jnp.int32, (rows, 1), 0)
    valid = jnp.where((position < live_rows) & (alive == 1), 1.0, 0.0).astype(jnp.float32)
    diff = keys - teacher.astype(jnp.float32)
    own_sum = jnp.sum(valid * diff * diff)
    upstream = (SCALE / total_count * valid * diff).astype(jnp.bfloat16)

    near_in = [near_half[0]] + [fetch(near_half[4 - s], Y, s) for s in (1, 2, 3)]
    far_in = [far_half[0]] + [fetch(far_half[4 - s], X, s) for s in (1, 2, 3)]
    near_up = ring_blocks(upstream, Y)
    far_up = ring_blocks(upstream, X)
    near_two = [fetch(block, C, 1) for block in near_up]
    far_two = near_two[:1] + [fetch(block, C, 1) for block in far_up[1:]]

    def pooled(left, up, two):
        products = [
            jnp.dot(left[i], jnp.concatenate([up[i], two[i]]), preferred_element_type=jnp.float32)
            for i in (0, 1, 3, 2)
        ]
        return sum(products).reshape(4, part, features)

    near_out = rolled(pooled(near_in, near_up, near_two), x)
    far_out = pooled(far_in, far_up, far_two)
    near_sum = near_out[0] + sum(fetch(near_out[4 - s], X, s) for s in (1, 2, 3))
    far_sum = far_out[0] + sum(fetch(far_out[4 - s], Y, s) for s in (1, 2, 3))
    both = jnp.where(zh == 0, jnp.stack([near_sum, far_sum]), jnp.stack([far_sum, near_sum]))

    half, side = part // 2, features // 2
    pieces = both.reshape(2, 2, half, 2, side).transpose(0, 1, 3, 2, 4).reshape(8, half, side)
    pieces = lax.all_to_all(pieces, (ZH, ZL), split_axis=0, concat_axis=0, tiled=True)
    whole = from_everyone(pieces.sum(axis=0), DP).reshape(2, 2, 4, half, side)
    grad_key = whole.transpose(2, 0, 3, 1, 4).reshape(own, features)
    grad_gain = jnp.sum(w_key.astype(jnp.float32) * grad_key, axis=1) / norm_gain.astype(jnp.float32)

    total_sum = summed(summed(own_sum, SHARD), DP)
    loss = total_sum / (2.0 * features * total_count)
    return (loss, grad_gain, grad_key)


def solution(mesh):
    split = Mesh(mesh.devices.reshape(4, 4, 2, 4, 2), DP_SHARD)
    return jax.shard_map(
        body,
        mesh=split,
        in_specs=(
            P(DP_SHARD, None),
            P(DP_SHARD, None),
            P(SHARD),
            P(SHARD, None),
            P(DP),
            P(DP, SHARD),
        ),
        out_specs=(P(), P(SHARD), P(SHARD, None)),
        check_vma=False,
    )
```

```python
import jax
import jax.numpy as jnp
from jax import lax
from jax.sharding import Mesh
from jax.sharding import PartitionSpec as P

ZL, X, ZH, Y, C = "dp_0", "dp_1", "shard_0", "shard_1", "shard_2"
SHARD = (ZH, Y, C)
DP_SHARD = (ZL, X, ZH, Y, C)
DP = (ZL, X)

EPSILON = 1e-06
SCALE = 1024.0


def fetch(value, axis, step):
    n = lax.axis_size(axis)
    return lax.ppermute(value, axis, [((i + step) % n, i) for i in range(n)])


def ring_blocks(value, axis):
    one, three, two = (fetch(value, axis, step) for step in (1, 3, 2))
    return [value, one, two, three]


def from_everyone(value, axes):
    copies = jnp.broadcast_to(value, (lax.axis_size(axes), *value.shape))
    return lax.all_to_all(copies, axes, split_axis=0, concat_axis=0, tiled=True)


def summed(value, axes):
    tile = jnp.broadcast_to(value, (8, 128))
    return from_everyone(tile, axes)[:, 0, 0].sum()


def block(value, *places):
    starts = [0 if at is None else at for at in places] + [0] * (value.ndim - len(places))
    sizes = [size if at is None else 1 for at, size in zip(places, value.shape)] + list(value.shape[len(places) :])
    kept = [size for at, size in zip(places, value.shape) if at is None] + list(value.shape[len(places) :])
    return lax.dynamic_slice(value, starts, sizes).reshape(kept)


def rows_by(left, right):
    return lax.dot_general(left, right, (((0,), (0,)), ((), ())), preferred_element_type=jnp.float32)


def body(hidden_in, teacher, norm_gain, w_key, group_rows, member):
    rows, width = hidden_in.shape
    own, features = w_key.shape
    part = own // 4
    x, y, zh, core = (lax.axis_index(name) for name in (X, Y, ZH, C))

    other = fetch(lax.dynamic_slice_in_dim(w_key, x * part, part), ZH, 1)
    near = ring_blocks(w_key, Y)
    quarter = jnp.zeros((4, part, features), w_key.dtype)
    for step, piece in enumerate(ring_blocks(other, Y)):
        quarter = lax.dynamic_update_index_in_dim(quarter, piece, (y + step) & 3, 0)
    far = [block.reshape(own, features) for block in ring_blocks(quarter, X)]

    live_rows = group_rows[0]
    alive = member[0, 0]
    own_count = (alive * live_rows).astype(jnp.float32)
    gain_rows = jnp.pad(norm_gain.astype(jnp.float32), (0, 384 - own)).reshape(3, 128)
    tile = jnp.concatenate([gain_rows, jnp.broadcast_to(own_count, (5, 128))])
    tiles = from_everyone(tile, SHARD)
    gains = tiles[:, :3].reshape(-1, 384)[:, :own].reshape(width)
    total_count = summed(tiles[:, 3, 0].sum(), DP)

    values = hidden_in.astype(jnp.float32)
    inverse_rms = lax.rsqrt(jnp.mean(values * values, axis=1, keepdims=True) + EPSILON)
    normed = (values * inverse_rms * gains).astype(jnp.bfloat16)

    turned = normed.T.reshape(2, 4, 2, 4, part, rows)
    theirs = fetch(block(turned, None, None, 1 - core), C, 1)
    pair = jnp.concatenate([block(turned, None, None, core), theirs], axis=-1)
    near_half = [block(pair, zh, (y + s) & 3).reshape(own, -1) for s in range(4)]
    far_half = [block(pair, 1 - zh, None, (x + s) & 3).reshape(own, -1) for s in range(4)]
    near_cols = [block(turned, zh, (y + s) & 3).reshape(2 * own, rows) for s in range(4)]
    far_cols = [block(turned, 1 - zh, None, None, (x + s) & 3).reshape(2 * own, rows) for s in range(4)]

    halves = rows_by(jnp.concatenate(near_half), jnp.concatenate(near)) + rows_by(far_half[0], far[0])
    halves += sum(rows_by(far_half[i], far[i]) for i in (1, 3, 2))
    keys = halves[:rows] + fetch(halves[rows:], C, 1)

    position = lax.broadcasted_iota(jnp.int32, (rows, 1), 0)
    valid = jnp.where((position < live_rows) & (alive == 1), 1.0, 0.0).astype(jnp.float32)
    diff = keys - teacher.astype(jnp.float32)
    own_sum = jnp.sum(valid * diff * diff)
    upstream = (SCALE / total_count * valid * diff).astype(jnp.bfloat16)

    near_in = [near_cols[0]] + [fetch(near_cols[4 - s], Y, s) for s in (1, 2, 3)]
    far_in = [far_cols[0]] + [fetch(far_cols[4 - s], X, s) for s in (1, 2, 3)]
    near_up = ring_blocks(upstream, Y)
    far_up = ring_blocks(upstream, X)

    def pooled(left, up):
        first = jnp.dot(
            jnp.concatenate([left[i] for i in (0, 1, 3)], axis=1),
            jnp.concatenate([up[i] for i in (0, 1, 3)]),
            preferred_element_type=jnp.float32,
        )
        return first + jnp.dot(left[2], up[2], preferred_element_type=jnp.float32)

    near_out = pooled(near_in, near_up).reshape(2, 4, part, features)
    near_out = block(near_out, core) + fetch(block(near_out, 1 - core), C, 1)
    far_out = pooled(far_in, far_up).reshape(4, 2, part, features)
    far_out = block(far_out, None, core) + fetch(block(far_out, None, 1 - core), C, 1)
    near_sum = block(near_out, x) + sum(fetch(block(near_out, (x - s) & 3), X, s) for s in (1, 2, 3))
    far_sum = block(far_out, y) + sum(fetch(block(far_out, (y - s) & 3), Y, s) for s in (1, 2, 3))
    both = jnp.where(zh == 0, jnp.stack([near_sum, far_sum]), jnp.stack([far_sum, near_sum]))

    tall, wide = part // 16, features // 256
    pieces = both.reshape(2, 2, tall, 8, 2, wide, 128).transpose(0, 1, 4, 2, 5, 3, 6).reshape(8, -1, 128)
    pieces = lax.all_to_all(pieces, (ZH, ZL), split_axis=0, concat_axis=0, tiled=True)
    group_sum = summed(own_sum, SHARD)
    piece = jnp.concatenate([pieces.sum(axis=0), jnp.broadcast_to(group_sum, (8, 128))])
    whole = from_everyone(piece, DP)
    loss = whole[:, -8, 0].sum() / (2.0 * features * total_count)
    whole = whole[:, :-8].reshape(2, 2, 4, tall, wide, 8, 128)
    grad_key = whole.transpose(2, 0, 3, 5, 1, 4, 6).reshape(own, features)
    grad_gain = jnp.sum(w_key.astype(jnp.float32) * grad_key, axis=1) / norm_gain.astype(jnp.float32)
    return (loss, grad_gain, grad_key)


def solution(mesh):
    split = Mesh(mesh.devices.reshape(4, 4, 2, 4, 2), DP_SHARD)
    return jax.shard_map(
        body,
        mesh=split,
        in_specs=(
            P(DP_SHARD, None),
            P(DP_SHARD, None),
            P(SHARD),
            P(SHARD, None),
            P(DP),
            P(DP, SHARD),
        ),
        out_specs=(P(), P(SHARD), P(SHARD, None)),
        check_vma=False,
    )
```

```python
import jax
import jax.numpy as jnp
from jax import lax
from jax.sharding import Mesh
from jax.sharding import PartitionSpec as P

ZL, X, ZH, Y, C = "dp_0", "dp_1", "shard_0", "shard_1", "shard_2"
SHARD = (ZH, Y, C)
DP_SHARD = (ZL, X, ZH, Y, C)
DP = (ZL, X)

EPSILON = 1e-06
SCALE = 1024.0


def fetch(value, axis, step):
    n = lax.axis_size(axis)
    return lax.ppermute(value, axis, [((i + step) % n, i) for i in range(n)])


def ring_blocks(value, axis):
    one, three, two = (fetch(value, axis, step) for step in (1, 3, 2))
    return [value, one, two, three]


def from_everyone(value, axes):
    copies = jnp.broadcast_to(value, (lax.axis_size(axes), *value.shape))
    return lax.all_to_all(copies, axes, split_axis=0, concat_axis=0, tiled=True)


def summed(value, axes):
    tile = jnp.broadcast_to(value, (8, 128))
    return from_everyone(tile, axes)[:, 0, 0].sum()


def block(value, *places):
    starts = [0 if at is None else at for at in places] + [0] * (value.ndim - len(places))
    sizes = [size if at is None else 1 for at, size in zip(places, value.shape)] + list(value.shape[len(places) :])
    kept = [size for at, size in zip(places, value.shape) if at is None] + list(value.shape[len(places) :])
    return lax.dynamic_slice(value, starts, sizes).reshape(kept)


def rows_by(left, right):
    return lax.dot_general(left, right, (((0,), (0,)), ((), ())), preferred_element_type=jnp.float32)


def body(hidden_in, teacher, norm_gain, w_key, group_rows, member):
    rows, width = hidden_in.shape
    own, features = w_key.shape
    part = own // 4
    x, y, zh, core = (lax.axis_index(name) for name in (X, Y, ZH, C))

    other = fetch(lax.dynamic_slice_in_dim(w_key, x * part, part), ZH, 1)
    near = ring_blocks(w_key, Y)
    quarter = jnp.zeros((4, part, features), w_key.dtype)
    for step, piece in enumerate(ring_blocks(other, Y)):
        quarter = lax.dynamic_update_index_in_dim(quarter, piece, (y + step) & 3, 0)
    far = [block.reshape(own, features) for block in ring_blocks(quarter, X)]

    live_rows = group_rows[0]
    alive = member[0, 0]
    own_count = (alive * live_rows).astype(jnp.float32)
    gain_rows = jnp.pad(norm_gain.astype(jnp.float32), (0, 384 - own)).reshape(3, 128)
    tile = jnp.concatenate([gain_rows, jnp.broadcast_to(own_count, (5, 128))])
    tiles = from_everyone(tile, SHARD)
    gains = tiles[:, :3].reshape(-1, 384)[:, :own].reshape(width)
    total_count = summed(tiles[:, 3, 0].sum(), DP)

    values = hidden_in.astype(jnp.float32)
    inverse_rms = lax.rsqrt(jnp.mean(values * values, axis=1, keepdims=True) + EPSILON)
    normed = (values * inverse_rms * gains).astype(jnp.bfloat16)

    turned = normed.T.reshape(2, 4, 2, 4, part, rows)
    theirs = fetch(block(turned, None, None, 1 - core), C, 1)
    pair = jnp.concatenate([block(turned, None, None, core), theirs], axis=-1)
    near_half = [block(pair, zh, (y + s) & 3).reshape(own, -1) for s in range(4)]
    far_half = [block(pair, 1 - zh, None, (x + s) & 3).reshape(own, -1) for s in range(4)]
    near_cols = [block(turned, zh, (y + s) & 3).reshape(2 * own, rows) for s in range(4)]
    far_cols = [block(turned, 1 - zh, None, None, (x + s) & 3).reshape(2 * own, rows) for s in range(4)]

    halves = rows_by(jnp.concatenate(near_half), jnp.concatenate(near)) + rows_by(far_half[0], far[0])
    halves += sum(rows_by(far_half[i], far[i]) for i in (1, 3, 2))
    keys = halves[:rows] + fetch(halves[rows:], C, 1)

    position = lax.broadcasted_iota(jnp.int32, (rows, 1), 0)
    valid = jnp.where((position < live_rows) & (alive == 1), 1.0, 0.0).astype(jnp.float32)
    diff = keys - teacher.astype(jnp.float32)
    own_sum = jnp.sum(valid * diff * diff)
    upstream = (SCALE / total_count * valid * diff).astype(jnp.bfloat16)

    near_in = [near_cols[0]] + [fetch(near_cols[4 - s], Y, s) for s in (1, 2, 3)]
    far_in = [far_cols[0]] + [fetch(far_cols[4 - s], X, s) for s in (1, 2, 3)]
    near_up = ring_blocks(upstream, Y)
    far_up = ring_blocks(upstream, X)

    def pooled(left, up):
        first = jnp.dot(
            jnp.concatenate([left[i] for i in (0, 1, 3)], axis=1),
            jnp.concatenate([up[i] for i in (0, 1, 3)]),
            preferred_element_type=jnp.float32,
        )
        first = lax.optimization_barrier(first)
        return first + jnp.dot(left[2], up[2], preferred_element_type=jnp.float32)

    near_out = pooled(near_in, near_up).reshape(2, 4, part, features)
    near_out = block(near_out, core) + fetch(block(near_out, 1 - core), C, 1)
    far_out = pooled(far_in, far_up).reshape(4, 2, part, features)
    far_out = block(far_out, None, core) + fetch(block(far_out, None, 1 - core), C, 1)
    near_sum = block(near_out, x) + sum(fetch(block(near_out, (x - s) & 3), X, s) for s in (1, 2, 3))
    far_sum = block(far_out, y) + sum(fetch(block(far_out, (y - s) & 3), Y, s) for s in (1, 2, 3))
    both = jnp.where(zh == 0, jnp.stack([near_sum, far_sum]), jnp.stack([far_sum, near_sum]))

    tall, wide = part // 16, features // 256

    def tiled(value):
        return value.reshape(-1, 2, tall, 8, 2, wide, 128).transpose(0, 1, 4, 2, 5, 3, 6)

    plane_sum = summed(own_sum, (X, Y, C))
    pieces = tiled(both).reshape(8, -1, 128)
    pieces = jnp.concatenate([pieces, jnp.broadcast_to(plane_sum, (8, 8, 128))], axis=1)
    pieces = lax.all_to_all(pieces, (ZH, ZL), split_axis=0, concat_axis=0, tiled=True).sum(axis=0)
    loss = pieces[-1, 0] / (2.0 * features * total_count)
    whole = from_everyone(pieces[:-8], DP).reshape(2, 2, 4, tall, wide, 8, 128)
    grad_key = whole.transpose(2, 0, 3, 5, 1, 4, 6).reshape(own, features)
    grad_gain = jnp.sum(w_key.astype(jnp.float32) * grad_key, axis=1) / norm_gain.astype(jnp.float32)
    return (loss, grad_gain, grad_key)


def solution(mesh):
    split = Mesh(mesh.devices.reshape(4, 4, 2, 4, 2), DP_SHARD)
    return jax.shard_map(
        body,
        mesh=split,
        in_specs=(
            P(DP_SHARD, None),
            P(DP_SHARD, None),
            P(SHARD),
            P(SHARD, None),
            P(DP),
            P(DP, SHARD),
        ),
        out_specs=(P(), P(SHARD), P(SHARD, None)),
        check_vma=False,
    )
```

```python
import jax
import jax.numpy as jnp
from jax import lax
from jax.sharding import Mesh
from jax.sharding import PartitionSpec as P

ZL, X, ZH, Y, C = "dp_0", "dp_1", "shard_0", "shard_1", "shard_2"
SHARD = (ZH, Y, C)
DP_SHARD = (ZL, X, ZH, Y, C)
DP = (ZL, X)

EPSILON = 1e-06
SCALE = 1024.0


def fetch(value, axis, step):
    n = lax.axis_size(axis)
    return lax.ppermute(value, axis, [((i + step) % n, i) for i in range(n)])


def ring_blocks(value, axis):
    one, three, two = (fetch(value, axis, step) for step in (1, 3, 2))
    return [value, one, two, three]


def from_everyone(value, axes):
    copies = jnp.broadcast_to(value, (lax.axis_size(axes), *value.shape))
    return lax.all_to_all(copies, axes, split_axis=0, concat_axis=0, tiled=True)


def summed(value, axes):
    tile = jnp.broadcast_to(value, (8, 128))
    return from_everyone(tile, axes)[:, 0, 0].sum()


def block(value, *places):
    starts = [0 if at is None else at for at in places] + [0] * (value.ndim - len(places))
    sizes = [size if at is None else 1 for at, size in zip(places, value.shape)] + list(value.shape[len(places) :])
    kept = [size for at, size in zip(places, value.shape) if at is None] + list(value.shape[len(places) :])
    return lax.dynamic_slice(value, starts, sizes).reshape(kept)


def rows_by(left, right):
    return lax.dot_general(left, right, (((0,), (0,)), ((), ())), preferred_element_type=jnp.float32)


def body(hidden_in, teacher, norm_gain, w_key, group_rows, member):
    rows, width = hidden_in.shape
    own, features = w_key.shape
    part = own // 4
    x, y, zh, core = (lax.axis_index(name) for name in (X, Y, ZH, C))

    other = fetch(lax.dynamic_slice_in_dim(w_key, x * part, part), ZH, 1)
    near = ring_blocks(w_key, Y)
    quarter = jnp.zeros((4, part, features), w_key.dtype)
    for step, piece in enumerate(ring_blocks(other, Y)):
        quarter = lax.dynamic_update_index_in_dim(quarter, piece, (y + step) & 3, 0)
    far = [block.reshape(own, features) for block in ring_blocks(quarter, X)]

    live_rows = group_rows[0]
    alive = member[0, 0]
    own_count = (alive * live_rows).astype(jnp.float32)
    gain_rows = jnp.pad(norm_gain.astype(jnp.float32), (0, 384 - own)).reshape(3, 128)
    tile = jnp.concatenate([gain_rows, jnp.broadcast_to(own_count, (5, 128))])
    tiles = from_everyone(tile, SHARD)
    gains = tiles[:, :3].reshape(-1, 384)[:, :own].reshape(width)
    total_count = summed(tiles[:, 3, 0].sum(), DP)

    values = hidden_in.astype(jnp.float32)
    inverse_rms = lax.rsqrt(jnp.mean(values * values, axis=1, keepdims=True) + EPSILON)
    normed = (values * inverse_rms * gains).astype(jnp.bfloat16)

    turned = normed.T.reshape(2, 4, 2, 4, part, rows)
    theirs = fetch(block(turned, None, None, 1 - core), C, 1)
    pair = jnp.concatenate([block(turned, None, None, core), theirs], axis=-1)
    near_half = [block(pair, zh, (y + s) & 3).reshape(own, -1) for s in range(4)]
    far_half = [block(pair, 1 - zh, None, (x + s) & 3).reshape(own, -1) for s in range(4)]
    near_cols = [block(turned, zh, (y + s) & 3).reshape(2 * own, rows) for s in range(4)]
    far_cols = [block(turned, 1 - zh, None, None, (x + s) & 3).reshape(2 * own, rows) for s in range(4)]

    halves = rows_by(jnp.concatenate(near_half), jnp.concatenate(near)) + rows_by(far_half[0], far[0])
    halves += sum(rows_by(far_half[i], far[i]) for i in (1, 3, 2))
    keys = halves[:rows] + fetch(halves[rows:], C, 1)

    position = lax.broadcasted_iota(jnp.int32, (rows, 1), 0)
    valid = jnp.where((position < live_rows) & (alive == 1), 1.0, 0.0).astype(jnp.float32)
    diff = keys - teacher.astype(jnp.float32)
    own_sum = jnp.sum(valid * diff * diff)
    upstream = (SCALE / total_count * valid * diff).astype(jnp.bfloat16)

    near_in = [near_cols[0]] + [fetch(near_cols[4 - s], Y, s) for s in (1, 2, 3)]
    far_in = [far_cols[0]] + [fetch(far_cols[4 - s], X, s) for s in (1, 2, 3)]
    near_up = ring_blocks(upstream, Y)
    far_up = ring_blocks(upstream, X)

    def pooled(left, up):
        first = jnp.dot(
            jnp.concatenate([left[i] for i in (0, 1, 3)], axis=1),
            jnp.concatenate([up[i] for i in (0, 1, 3)]),
            preferred_element_type=jnp.float32,
        )
        first = lax.optimization_barrier(first)
        return first + jnp.dot(left[2], up[2], preferred_element_type=jnp.float32)

    near_out = pooled(near_in, near_up).reshape(2, 4, part, features)
    near_out = block(near_out, core) + fetch(block(near_out, 1 - core), C, 1)
    far_out = pooled(far_in, far_up).reshape(4, 2, part, features)
    far_out = block(far_out, None, core) + fetch(block(far_out, None, 1 - core), C, 1)
    near_sum = block(near_out, x) + sum(fetch(block(near_out, (x - s) & 3), X, s) for s in (1, 2, 3))
    far_sum = block(far_out, y) + sum(fetch(block(far_out, (y - s) & 3), Y, s) for s in (1, 2, 3))
    both = jnp.where(zh == 0, jnp.stack([near_sum, far_sum]), jnp.stack([far_sum, near_sum]))

    tall, wide = part // 16, features // 256

    def tiled(value):
        return value.reshape(-1, 2, tall, 8, 2, wide, 128).transpose(0, 1, 4, 2, 5, 3, 6)

    plane_sum = summed(own_sum, (X, Y, C))
    pieces = tiled(both).reshape(8, -1, 128)
    pieces = jnp.concatenate([pieces, jnp.broadcast_to(plane_sum, (8, 8, 128))], axis=1)
    pieces = lax.all_to_all(pieces, (ZH, ZL), split_axis=0, concat_axis=0, tiled=True).sum(axis=0)
    loss = pieces[-1, 0] / (2.0 * features * total_count)

    piece = pieces[:-8]
    mine = tiled(block(w_key.reshape(4, part, features), x)).reshape(4, -1, 128)
    share = (piece * block(mine, lax.axis_index(ZL)).astype(jnp.float32)).sum(axis=1)
    lines = []
    for _ in range(3):
        lines.append(lax.reduce_precision(share, 8, 7))
        share = share - lines[-1]
    lines = jnp.pad(jnp.stack(lines), ((0, 5), (0, 128 - share.size)))
    whole = from_everyone(jnp.concatenate([piece, lines]).astype(jnp.bfloat16), DP)
    shares = whole[:, -8:-5, : share.size].astype(jnp.float32).sum(axis=1).reshape(2, 2, 4, tall, wide, 8)
    grad_gain = shares.sum(axis=(1, 4)).swapaxes(0, 1).reshape(own) / norm_gain.astype(jnp.float32)
    whole = whole[:, :-8].reshape(2, 2, 4, tall, wide, 8, 128)
    grad_key = whole.transpose(2, 0, 3, 5, 1, 4, 6).reshape(own, features).astype(jnp.float32)
    return (loss, grad_gain, grad_key)


def solution(mesh):
    split = Mesh(mesh.devices.reshape(4, 4, 2, 4, 2), DP_SHARD)
    return jax.shard_map(
        body,
        mesh=split,
        in_specs=(
            P(DP_SHARD, None),
            P(DP_SHARD, None),
            P(SHARD),
            P(SHARD, None),
            P(DP),
            P(DP, SHARD),
        ),
        out_specs=(P(), P(SHARD), P(SHARD, None)),
        check_vma=False,
    )
```

```python
import jax
import jax.numpy as jnp
from jax import lax
from jax.sharding import Mesh
from jax.sharding import PartitionSpec as P

ZL, X, ZH, Y, C = "dp_0", "dp_1", "shard_0", "shard_1", "shard_2"
SHARD = (ZH, Y, C)
DP_SHARD = (ZL, X, ZH, Y, C)
DP = (ZL, X)

EPSILON = 1e-06
SCALE = 1024.0


def fetch(value, axis, step):
    n = lax.axis_size(axis)
    return lax.ppermute(value, axis, [((i + step) % n, i) for i in range(n)])


def ring_blocks(value, axis, relay=True):
    one, three = (fetch(value, axis, step) for step in (1, 3))
    two = fetch(one, axis, 1) if relay else fetch(value, axis, 2)
    return [value, one, two, three]


def from_everyone(value, axes):
    copies = jnp.broadcast_to(value, (lax.axis_size(axes), *value.shape))
    return lax.all_to_all(copies, axes, split_axis=0, concat_axis=0, tiled=True)


def summed(value, axes):
    tile = jnp.broadcast_to(value, (8, 128))
    return from_everyone(tile, axes)[:, 0, 0].sum()


def block(value, *places):
    starts = [0 if at is None else at for at in places] + [0] * (value.ndim - len(places))
    sizes = [size if at is None else 1 for at, size in zip(places, value.shape)] + list(value.shape[len(places) :])
    kept = [size for at, size in zip(places, value.shape) if at is None] + list(value.shape[len(places) :])
    return lax.dynamic_slice(value, starts, sizes).reshape(kept)


def rows_by(left, right):
    return lax.dot_general(left, right, (((0,), (0,)), ((), ())), preferred_element_type=jnp.float32)


def body(hidden_in, teacher, norm_gain, w_key, group_rows, member):
    rows, width = hidden_in.shape
    own, features = w_key.shape
    part = own // 4
    x, y, zh, core = (lax.axis_index(name) for name in (X, Y, ZH, C))

    other = fetch(lax.dynamic_slice_in_dim(w_key, x * part, part), ZH, 1)
    near = ring_blocks(w_key, Y)
    quarter = jnp.zeros((4, part, features), w_key.dtype)
    for step, piece in enumerate(ring_blocks(other, Y, relay=False)):
        quarter = lax.dynamic_update_index_in_dim(quarter, piece, (y + step) & 3, 0)
    far = [block.reshape(own, features) for block in ring_blocks(quarter, X)]

    live_rows = group_rows[0]
    alive = member[0, 0]
    own_count = (alive * live_rows).astype(jnp.float32)
    gain_rows = jnp.pad(norm_gain.astype(jnp.float32), (0, 384 - own)).reshape(3, 128)
    tile = jnp.concatenate([gain_rows, jnp.broadcast_to(own_count, (5, 128))])
    tiles = from_everyone(tile, SHARD)
    gains = tiles[:, :3].reshape(-1, 384)[:, :own].reshape(width)
    total_count = summed(tiles[:, 3, 0].sum(), DP)

    values = hidden_in.astype(jnp.float32)
    inverse_rms = lax.rsqrt(jnp.mean(values * values, axis=1, keepdims=True) + EPSILON)
    normed = (values * inverse_rms * gains).astype(jnp.bfloat16)

    turned = normed.T.reshape(2, 4, 2, 4, part, rows)
    theirs = fetch(block(turned, None, None, 1 - core), C, 1)
    pair = jnp.concatenate([block(turned, None, None, core), theirs], axis=-1)
    near_half = [block(pair, zh, (y + s) & 3).reshape(own, -1) for s in range(4)]
    far_half = [block(pair, 1 - zh, None, (x + s) & 3).reshape(own, -1) for s in range(4)]
    near_cols = [block(turned, zh, (y + s) & 3).reshape(2 * own, rows) for s in range(4)]
    far_cols = [block(turned, 1 - zh, None, None, (x + s) & 3).reshape(2 * own, rows) for s in range(4)]

    halves = rows_by(jnp.concatenate(near_half), jnp.concatenate(near)) + rows_by(far_half[0], far[0])
    halves += sum(rows_by(far_half[i], far[i]) for i in (1, 3, 2))
    keys = halves[:rows] + fetch(halves[rows:], C, 1)

    position = lax.broadcasted_iota(jnp.int32, (rows, 1), 0)
    valid = jnp.where((position < live_rows) & (alive == 1), 1.0, 0.0).astype(jnp.float32)
    diff = keys - teacher.astype(jnp.float32)
    own_sum = jnp.sum(valid * diff * diff)
    upstream = (SCALE / total_count * valid * diff).astype(jnp.bfloat16)

    near_in = [near_cols[0]] + [fetch(near_cols[4 - s], Y, s) for s in (1, 2, 3)]
    far_in = [far_cols[0]] + [fetch(far_cols[4 - s], X, s) for s in (1, 2, 3)]
    near_up = ring_blocks(upstream, Y)
    far_up = ring_blocks(upstream, X)

    def pooled(left, up):
        first = jnp.dot(
            jnp.concatenate([left[i] for i in (0, 1, 3)], axis=1),
            jnp.concatenate([up[i] for i in (0, 1, 3)]),
            preferred_element_type=jnp.float32,
        )
        first = lax.optimization_barrier(first)
        return first + jnp.dot(left[2], up[2], preferred_element_type=jnp.float32)

    near_out = pooled(near_in, near_up).reshape(2, 4, part, features)
    near_out = block(near_out, core) + fetch(block(near_out, 1 - core), C, 1)
    far_out = pooled(far_in, far_up).reshape(4, 2, part, features)
    far_out = block(far_out, None, core) + fetch(block(far_out, None, 1 - core), C, 1)
    near_sum = block(near_out, x) + sum(fetch(block(near_out, (x - s) & 3), X, s) for s in (1, 2, 3))
    far_sum = block(far_out, y) + sum(fetch(block(far_out, (y - s) & 3), Y, s) for s in (1, 2, 3))
    both = jnp.where(zh == 0, jnp.stack([near_sum, far_sum]), jnp.stack([far_sum, near_sum]))

    tall, wide = part // 16, features // 256

    def tiled(value):
        return value.reshape(-1, 2, tall, 8, 2, wide, 128).transpose(0, 1, 4, 2, 5, 3, 6)

    plane_sum = summed(own_sum, (X, Y, C))
    pieces = tiled(both).reshape(8, -1, 128)
    pieces = jnp.concatenate([pieces, jnp.broadcast_to(plane_sum, (8, 8, 128))], axis=1)
    pieces = lax.all_to_all(pieces, (ZH, ZL), split_axis=0, concat_axis=0, tiled=True).sum(axis=0)
    loss = pieces[-1, 0] / (2.0 * features * total_count)

    piece = pieces[:-8]
    mine = tiled(block(w_key.reshape(4, part, features), x)).reshape(4, -1, 128)
    share = (piece * block(mine, lax.axis_index(ZL)).astype(jnp.float32)).sum(axis=1)
    lines = []
    for _ in range(3):
        lines.append(lax.reduce_precision(share, 8, 7))
        share = share - lines[-1]
    lines = jnp.pad(jnp.stack(lines), ((0, 5), (0, 128 - share.size)))
    whole = from_everyone(jnp.concatenate([piece, lines]).astype(jnp.bfloat16), DP)
    shares = whole[:, -8:-5, : share.size].astype(jnp.float32).sum(axis=1).reshape(2, 2, 4, tall, wide, 8)
    grad_gain = shares.sum(axis=(1, 4)).swapaxes(0, 1).reshape(own) / norm_gain.astype(jnp.float32)
    whole = whole[:, :-8].reshape(2, 2, 4, tall, wide, 8, 128)
    grad_key = whole.transpose(2, 0, 3, 5, 1, 4, 6).reshape(own, features).astype(jnp.float32)
    return (loss, grad_gain, grad_key)


def solution(mesh):
    split = Mesh(mesh.devices.reshape(4, 4, 2, 4, 2), DP_SHARD)
    return jax.shard_map(
        body,
        mesh=split,
        in_specs=(
            P(DP_SHARD, None),
            P(DP_SHARD, None),
            P(SHARD),
            P(SHARD, None),
            P(DP),
            P(DP, SHARD),
        ),
        out_specs=(P(), P(SHARD), P(SHARD, None)),
        check_vma=False,
    )
```

```python
import jax
import jax.numpy as jnp
from jax import lax
from jax.sharding import Mesh
from jax.sharding import PartitionSpec as P

ZL, X, ZH, Y, C = "dp_0", "dp_1", "shard_0", "shard_1", "shard_2"
SHARD = (ZH, Y, C)
DP_SHARD = (ZL, X, ZH, Y, C)
DP = (ZL, X)

EPSILON = 1e-06
SCALE = 1024.0


def fetch(value, axis, step):
    n = lax.axis_size(axis)
    return lax.ppermute(value, axis, [((i + step) % n, i) for i in range(n)])


def ring_blocks(value, axis, relay=True):
    one, three = (fetch(value, axis, step) for step in (1, 3))
    two = fetch(one, axis, 1) if relay else fetch(value, axis, 2)
    return [value, one, two, three]


def from_everyone(value, axes):
    copies = jnp.broadcast_to(value, (lax.axis_size(axes), *value.shape))
    return lax.all_to_all(copies, axes, split_axis=0, concat_axis=0, tiled=True)


def summed(value, axes):
    tile = jnp.broadcast_to(value, (8, 128))
    return from_everyone(tile, axes)[:, 0, 0].sum()


def block(value, *places):
    starts = [0 if at is None else at for at in places] + [0] * (value.ndim - len(places))
    sizes = [size if at is None else 1 for at, size in zip(places, value.shape)] + list(value.shape[len(places) :])
    kept = [size for at, size in zip(places, value.shape) if at is None] + list(value.shape[len(places) :])
    return lax.dynamic_slice(value, starts, sizes).reshape(kept)


def rows_by(left, right):
    return lax.dot_general(left, right, (((0,), (0,)), ((), ())), preferred_element_type=jnp.float32)


def body(hidden_in, teacher, norm_gain, w_key, group_rows, member):
    rows, width = hidden_in.shape
    own, features = w_key.shape
    part = own // 4
    x, y, zh, core = (lax.axis_index(name) for name in (X, Y, ZH, C))

    other = fetch(lax.dynamic_slice_in_dim(w_key, x * part, part), ZH, 1)
    near = ring_blocks(w_key, Y)
    quarter = jnp.zeros((4, part, features), w_key.dtype)
    for step, piece in enumerate(ring_blocks(other, Y, relay=False)):
        quarter = lax.dynamic_update_index_in_dim(quarter, piece, (y + step) & 3, 0)
    far = [block.reshape(own, features) for block in ring_blocks(quarter, X)]

    live_rows = group_rows[0]
    alive = member[0, 0]
    own_count = (alive * live_rows).astype(jnp.float32)
    gain_rows = jnp.pad(norm_gain.astype(jnp.float32), (0, 384 - own)).reshape(3, 128)
    tile = jnp.concatenate([gain_rows, jnp.broadcast_to(own_count, (5, 128))])
    tiles = from_everyone(tile, SHARD)
    gains = tiles[:, :3].reshape(-1, 384)[:, :own].reshape(width)
    total_count = summed(tiles[:, 3, 0].sum(), DP)

    values = hidden_in.astype(jnp.float32)
    inverse_rms = lax.rsqrt(jnp.mean(values * values, axis=1, keepdims=True) + EPSILON)
    normed = (values * inverse_rms * gains).astype(jnp.bfloat16)

    turned = normed.T.reshape(2, 4, 2, 4, part, rows)
    own_cols, their_cols = block(turned, None, None, core), block(turned, None, None, 1 - core)
    pair = jnp.concatenate([own_cols, fetch(their_cols, C, 1)], axis=-1)
    near_half = [block(pair, zh, (y + s) & 3).reshape(own, -1) for s in range(4)]
    far_half = [block(pair, 1 - zh, None, (x + s) & 3).reshape(own, -1) for s in range(4)]
    near_cols = [block(turned, zh, (y + s) & 3).reshape(2 * own, rows) for s in range(4)]
    far_cols = [block(turned, 1 - zh, None, None, (x + s) & 3).reshape(2 * own, rows) for s in range(4)]

    halves = rows_by(jnp.concatenate(near_half), jnp.concatenate(near)) + rows_by(far_half[0], far[0])
    halves += sum(rows_by(far_half[i], far[i]) for i in (1, 3, 2))
    keys = halves[:rows] + fetch(halves[rows:], C, 1)

    position = lax.broadcasted_iota(jnp.int32, (rows, 1), 0)
    valid = jnp.where((position < live_rows) & (alive == 1), 1.0, 0.0).astype(jnp.float32)
    diff = keys - teacher.astype(jnp.float32)
    own_sum = jnp.sum(valid * diff * diff)
    upstream = (SCALE / total_count * valid * diff).astype(jnp.bfloat16)

    near_in = [near_cols[0]] + [fetch(near_cols[4 - s], Y, s) for s in (1, 2, 3)]
    far_in = [far_cols[0]] + [fetch(far_cols[4 - s], X, s) for s in (1, 2, 3)]
    near_up = ring_blocks(upstream, Y)
    far_up = ring_blocks(upstream, X)

    def pooled(left, up):
        first = jnp.dot(
            jnp.concatenate([left[i] for i in (0, 1, 3)], axis=1),
            jnp.concatenate([up[i] for i in (0, 1, 3)]),
            preferred_element_type=jnp.float32,
        )
        first = lax.optimization_barrier(first)
        return first + jnp.dot(left[2], up[2], preferred_element_type=jnp.float32)

    near_out = pooled(near_in, near_up).reshape(2, 4, part, features)
    near_out = block(near_out, core) + fetch(block(near_out, 1 - core), C, 1)
    far_out = pooled(far_in, far_up).reshape(4, 2, part, features)
    far_out = block(far_out, None, core) + fetch(block(far_out, None, 1 - core), C, 1)
    near_sum = block(near_out, x) + sum(fetch(block(near_out, (x - s) & 3), X, s) for s in (1, 2, 3))
    far_sum = block(far_out, y) + sum(fetch(block(far_out, (y - s) & 3), Y, s) for s in (1, 2, 3))
    both = jnp.where(zh == 0, jnp.stack([near_sum, far_sum]), jnp.stack([far_sum, near_sum]))

    tall, wide = part // 16, features // 256

    def tiled(value):
        return value.reshape(-1, 2, tall, 8, 2, wide, 128).transpose(0, 1, 4, 2, 5, 3, 6)

    near_loss = summed(own_sum, (Y, C))
    pieces = tiled(both).reshape(8, -1, 128)
    pieces = jnp.concatenate([pieces, jnp.broadcast_to(near_loss, (8, 8, 128))], axis=1)
    pieces = lax.all_to_all(pieces, (ZH, ZL), split_axis=0, concat_axis=0, tiled=True).sum(axis=0)

    piece = pieces[:-8]
    mine = tiled(block(w_key.reshape(4, part, features), x)).reshape(4, -1, 128)
    share = (piece * block(mine, lax.axis_index(ZL)).astype(jnp.float32)).sum(axis=1)
    share = jnp.concatenate([share, pieces[-1, :8]])
    lines = []
    for _ in range(3):
        lines.append(lax.reduce_precision(share, 8, 7))
        share = share - lines[-1]
    lines = jnp.pad(jnp.stack(lines), ((0, 5), (0, 0)))
    whole = from_everyone(jnp.concatenate([piece, lines]).astype(jnp.bfloat16), DP)
    shares = whole[:, -8:-5].astype(jnp.float32).sum(axis=1)
    loss = shares[:4, -1].sum() / (2.0 * features * total_count)
    shares = shares[:, :-8].reshape(2, 2, 4, tall, wide, 8)
    grad_gain = shares.sum(axis=(1, 4)).swapaxes(0, 1).reshape(own) / norm_gain.astype(jnp.float32)
    whole = whole[:, :-8].reshape(2, 2, 4, tall, wide, 8, 128)
    grad_key = whole.transpose(2, 0, 3, 5, 1, 4, 6).reshape(own, features).astype(jnp.float32)
    return (loss, grad_gain, grad_key)


def solution(mesh):
    split = Mesh(mesh.devices.reshape(4, 4, 2, 4, 2), DP_SHARD)
    return jax.shard_map(
        body,
        mesh=split,
        in_specs=(
            P(DP_SHARD, None),
            P(DP_SHARD, None),
            P(SHARD),
            P(SHARD, None),
            P(DP),
            P(DP, SHARD),
        ),
        out_specs=(P(), P(SHARD), P(SHARD, None)),
        check_vma=False,
    )
```

```python
import jax
import jax.numpy as jnp
from jax import lax
from jax.sharding import Mesh
from jax.sharding import PartitionSpec as P

ZL, X, ZH, Y, C = "dp_0", "dp_1", "shard_0", "shard_1", "shard_2"
SHARD = (ZH, Y, C)
DP_SHARD = (ZL, X, ZH, Y, C)
DP = (ZL, X)

EPSILON = 1e-06
SCALE = 1024.0


def fetch(value, axis, step):
    n = lax.axis_size(axis)
    return lax.ppermute(value, axis, [((i + step) % n, i) for i in range(n)])


def ring_blocks(value, axis, relay=True):
    one, three = (fetch(value, axis, step) for step in (1, 3))
    two = fetch(one, axis, 1) if relay else fetch(value, axis, 2)
    return [value, one, two, three]


def from_everyone(value, axes):
    copies = jnp.broadcast_to(value, (lax.axis_size(axes), *value.shape))
    return lax.all_to_all(copies, axes, split_axis=0, concat_axis=0, tiled=True)


def summed(value, axes):
    tile = jnp.broadcast_to(value, (8, 128))
    return from_everyone(tile, axes)[:, 0, 0].sum()


def block(value, *places):
    starts = [0 if at is None else at for at in places] + [0] * (value.ndim - len(places))
    sizes = [size if at is None else 1 for at, size in zip(places, value.shape)] + list(value.shape[len(places) :])
    kept = [size for at, size in zip(places, value.shape) if at is None] + list(value.shape[len(places) :])
    return lax.dynamic_slice(value, starts, sizes).reshape(kept)


def rows_by(left, right):
    return lax.dot_general(left, right, (((0,), (0,)), ((), ())), preferred_element_type=jnp.float32)


def body(hidden_in, teacher, norm_gain, w_key, group_rows, member):
    rows, width = hidden_in.shape
    own, features = w_key.shape
    part = own // 4
    x, y, zh, core = (lax.axis_index(name) for name in (X, Y, ZH, C))

    other = fetch(lax.dynamic_slice_in_dim(w_key, x * part, part), ZH, 1)
    near = ring_blocks(w_key, Y)
    quarter = jnp.zeros((4, part, features), w_key.dtype)
    for step, piece in enumerate(ring_blocks(other, Y, relay=False)):
        quarter = lax.dynamic_update_index_in_dim(quarter, piece, (y + step) & 3, 0)
    far = [block.reshape(own, features) for block in ring_blocks(quarter, X)]

    live_rows = group_rows[0]
    alive = member[0, 0]
    own_count = (alive * live_rows).astype(jnp.float32)
    gain_rows = jnp.pad(norm_gain.astype(jnp.float32), (0, 384 - own)).reshape(3, 128)
    tile = jnp.concatenate([gain_rows, jnp.broadcast_to(own_count, (5, 128))])
    tiles = from_everyone(tile, SHARD)
    gains = tiles[:, :3].reshape(-1, 384)[:, :own].reshape(width)
    total_count = summed(tiles[:, 3, 0].sum(), DP)

    values = hidden_in.astype(jnp.float32)
    inverse_rms = lax.rsqrt(jnp.mean(values * values, axis=1, keepdims=True) + EPSILON)
    normed = (values * inverse_rms * gains).astype(jnp.bfloat16)

    turned = normed.T.reshape(2, 4, 2, 4, part, rows)
    own_cols, their_cols = block(turned, None, None, core), block(turned, None, None, 1 - core)
    pair = jnp.concatenate([own_cols, fetch(their_cols, C, 1)], axis=-1)
    near_half = [block(pair, zh, (y + s) & 3).reshape(own, -1) for s in range(4)]
    far_half = [block(pair, 1 - zh, None, (x + s) & 3).reshape(own, -1) for s in range(4)]
    near_cols = [block(turned, zh, (y + s) & 3).reshape(2 * own, rows) for s in range(4)]
    far_cols = [block(turned, 1 - zh, None, None, (x + s) & 3).reshape(2 * own, rows) for s in range(4)]

    halves = rows_by(jnp.concatenate(near_half), jnp.concatenate(near)) + rows_by(far_half[0], far[0])
    halves += rows_by(jnp.concatenate([far_half[1], far_half[3]]), jnp.concatenate([far[1], far[3]]))
    halves += rows_by(far_half[2], far[2])
    keys = halves[:rows] + fetch(halves[rows:], C, 1)

    position = lax.broadcasted_iota(jnp.int32, (rows, 1), 0)
    valid = jnp.where((position < live_rows) & (alive == 1), 1.0, 0.0).astype(jnp.float32)
    diff = keys - teacher.astype(jnp.float32)
    own_sum = jnp.sum(valid * diff * diff)
    upstream = (SCALE / total_count * valid * diff).astype(jnp.bfloat16)

    near_in = [near_cols[0]] + [fetch(near_cols[4 - s], Y, s) for s in (1, 2, 3)]
    far_in = [far_cols[0]] + [fetch(far_cols[4 - s], X, s) for s in (1, 2, 3)]
    near_up = ring_blocks(upstream, Y)
    far_up = ring_blocks(upstream, X)

    def pooled(left, up, halve):
        first = jnp.dot(
            jnp.concatenate([left[i] for i in (0, 1, 3)], axis=1),
            jnp.concatenate([up[i] for i in (0, 1, 3)]),
            preferred_element_type=jnp.float32,
        )
        first = lax.optimization_barrier(first)
        return [
            halve(first, side) + jnp.dot(halve(left[2], side), up[2], preferred_element_type=jnp.float32)
            for side in (1 - core, core)
        ]

    def near_rows(value, side):
        return block(value.reshape(2, own, -1), side)

    def far_rows(value, side):
        return block(value.reshape(4, 2, part, -1), None, side).reshape(own, -1)

    near_other, near_mine = pooled(near_in, near_up, near_rows)
    far_other, far_mine = pooled(far_in, far_up, far_rows)
    near_out = (near_mine + fetch(near_other, C, 1)).reshape(4, part, features)
    far_out = (far_mine + fetch(far_other, C, 1)).reshape(4, part, features)
    near_sum = block(near_out, x) + sum(fetch(block(near_out, (x - s) & 3), X, s) for s in (1, 2, 3))
    far_sum = block(far_out, y) + sum(fetch(block(far_out, (y - s) & 3), Y, s) for s in (1, 2, 3))
    both = jnp.where(zh == 0, jnp.stack([near_sum, far_sum]), jnp.stack([far_sum, near_sum]))

    tall, wide = part // 16, features // 256

    def tiled(value):
        return value.reshape(-1, 2, tall, 8, 2, wide, 128).transpose(0, 1, 4, 2, 5, 3, 6)

    pieces = tiled(both).reshape(8, -1, 128)
    piece = lax.all_to_all(pieces, (ZH, ZL), split_axis=0, concat_axis=0, tiled=True).sum(axis=0)
    group_sum = summed(own_sum, SHARD)

    mine = tiled(block(w_key.reshape(4, part, features), x)).reshape(4, -1, 128)
    share = (piece * block(mine, lax.axis_index(ZL)).astype(jnp.float32)).sum(axis=1)
    share = jnp.concatenate([share, jnp.broadcast_to(group_sum, (8,))])
    lines = []
    for _ in range(3):
        lines.append(lax.reduce_precision(share, 8, 7))
        share = share - lines[-1]
    lines = jnp.pad(jnp.stack(lines), ((0, 5), (0, 0)))
    whole = from_everyone(jnp.concatenate([piece, lines]).astype(jnp.bfloat16), DP)
    shares = whole[:, -8:-5].astype(jnp.float32).sum(axis=1)
    loss = shares[:, -1].sum() / (2.0 * features * total_count)
    shares = shares[:, :-8].reshape(2, 2, 4, tall, wide, 8)
    grad_gain = shares.sum(axis=(1, 4)).swapaxes(0, 1).reshape(own) / norm_gain.astype(jnp.float32)
    whole = whole[:, :-8].reshape(2, 2, 4, tall, wide, 8, 128)
    grad_key = whole.transpose(2, 0, 3, 5, 1, 4, 6).reshape(own, features).astype(jnp.float32)
    return (loss, grad_gain, grad_key)


def solution(mesh):
    split = Mesh(mesh.devices.reshape(4, 4, 2, 4, 2), DP_SHARD)
    return jax.shard_map(
        body,
        mesh=split,
        in_specs=(
            P(DP_SHARD, None),
            P(DP_SHARD, None),
            P(SHARD),
            P(SHARD, None),
            P(DP),
            P(DP, SHARD),
        ),
        out_specs=(P(), P(SHARD), P(SHARD, None)),
        check_vma=False,
    )
```

```python
import jax
import jax.numpy as jnp
from jax import lax
from jax.sharding import Mesh
from jax.sharding import PartitionSpec as P

ZL, X, ZH, Y, C = "dp_0", "dp_1", "shard_0", "shard_1", "shard_2"
SHARD = (ZH, Y, C)
DP_SHARD = (ZL, X, ZH, Y, C)
DP = (ZL, X)

EPSILON = 1e-06
SCALE = 1024.0


def fetch(value, axis, step):
    n = lax.axis_size(axis)
    return lax.ppermute(value, axis, [((i + step) % n, i) for i in range(n)])


def ring_blocks(value, axis, relay=True):
    one, three = (fetch(value, axis, step) for step in (1, 3))
    two = fetch(one, axis, 1) if relay else fetch(value, axis, 2)
    return [value, one, two, three]


def from_everyone(value, axes):
    copies = jnp.broadcast_to(value, (lax.axis_size(axes), *value.shape))
    return lax.all_to_all(copies, axes, split_axis=0, concat_axis=0, tiled=True)


def summed(value, axes):
    tile = jnp.broadcast_to(value, (8, 128))
    return from_everyone(tile, axes)[:, 0, 0].sum()


def block(value, *places):
    starts = [0 if at is None else at for at in places] + [0] * (value.ndim - len(places))
    sizes = [size if at is None else 1 for at, size in zip(places, value.shape)] + list(value.shape[len(places) :])
    kept = [size for at, size in zip(places, value.shape) if at is None] + list(value.shape[len(places) :])
    return lax.dynamic_slice(value, starts, sizes).reshape(kept)


def rows_by(left, right):
    return lax.dot_general(left, right, (((0,), (0,)), ((), ())), preferred_element_type=jnp.float32)


def body(hidden_in, teacher, norm_gain, w_key, group_rows, member):
    rows, width = hidden_in.shape
    own, features = w_key.shape
    part = own // 4
    x, y, zh, core = (lax.axis_index(name) for name in (X, Y, ZH, C))

    other = fetch(lax.dynamic_slice_in_dim(w_key, x * part, part), ZH, 1)
    near = ring_blocks(w_key, Y)
    quarter = jnp.zeros((4, part, features), w_key.dtype)
    for step, piece in enumerate(ring_blocks(other, Y, relay=False)):
        quarter = lax.dynamic_update_index_in_dim(quarter, piece, (y + step) & 3, 0)
    far = [block.reshape(own, features) for block in ring_blocks(quarter, X)]

    live_rows = group_rows[0]
    alive = member[0, 0]
    own_count = (alive * live_rows).astype(jnp.float32)
    gain_rows = jnp.pad(norm_gain.astype(jnp.float32), (0, 384 - own)).reshape(3, 128)
    tile = jnp.concatenate([gain_rows, jnp.broadcast_to(own_count, (5, 128))])
    tiles = from_everyone(tile, SHARD)
    gains = tiles[:, :3].reshape(-1, 384)[:, :own].reshape(width)
    total_count = summed(tiles[:, 3, 0].sum(), DP)

    values = hidden_in.astype(jnp.float32)
    inverse_rms = lax.rsqrt(jnp.mean(values * values, axis=1, keepdims=True) + EPSILON)
    normed = (values * inverse_rms * gains).astype(jnp.bfloat16)

    turned = normed.T.reshape(2, 4, 2, 4, part, rows)
    own_cols, their_cols = block(turned, None, None, core), block(turned, None, None, 1 - core)
    pair = jnp.concatenate([own_cols, fetch(their_cols, C, 1)], axis=-1)
    near_half = [block(pair, zh, (y + s) & 3).reshape(own, -1) for s in range(4)]
    far_half = [block(pair, 1 - zh, None, (x + s) & 3).reshape(own, -1) for s in range(4)]
    near_cols = [block(turned, zh, (y + s) & 3).reshape(2 * own, rows) for s in range(4)]
    far_cols = [block(turned, 1 - zh, None, None, (x + s) & 3).reshape(2 * own, rows) for s in range(4)]

    halves = rows_by(jnp.concatenate(near_half), jnp.concatenate(near)) + rows_by(far_half[0], far[0])
    halves += rows_by(jnp.concatenate([far_half[1], far_half[3]]), jnp.concatenate([far[1], far[3]]))
    halves += rows_by(far_half[2], far[2])
    keys = halves[:rows] + fetch(halves[rows:], C, 1)

    position = lax.broadcasted_iota(jnp.int32, (rows, 1), 0)
    valid = jnp.where((position < live_rows) & (alive == 1), 1.0, 0.0).astype(jnp.float32)
    diff = keys - teacher.astype(jnp.float32)
    own_sum = jnp.sum(valid * diff * diff)
    upstream = (SCALE / total_count * valid * diff).astype(jnp.bfloat16)

    near_in = [near_cols[0]] + [fetch(near_cols[4 - s], Y, s) for s in (1, 2, 3)]
    far_in = [far_cols[0]] + [fetch(far_cols[4 - s], X, s) for s in (1, 2, 3)]
    near_up = ring_blocks(upstream, Y)
    far_up = ring_blocks(upstream, X)

    def pooled(left, up, halve):
        first = jnp.dot(
            jnp.concatenate([left[i] for i in (0, 1, 3)], axis=1),
            jnp.concatenate([up[i] for i in (0, 1, 3)]),
            preferred_element_type=jnp.float32,
        )
        first = lax.optimization_barrier(first)
        return [
            halve(first, side) + jnp.dot(halve(left[2], side), up[2], preferred_element_type=jnp.float32)
            for side in (1 - core, core)
        ]

    def near_rows(value, side):
        return block(value.reshape(2, own, -1), side)

    def far_rows(value, side):
        return block(value.reshape(4, 2, part, -1), None, side).reshape(own, -1)

    near_other, near_mine = pooled(near_in, near_up, near_rows)
    far_other, far_mine = pooled(far_in, far_up, far_rows)
    near_out = (near_mine + fetch(near_other, C, 1)).reshape(4, part, features)
    far_out = (far_mine + fetch(far_other, C, 1)).reshape(4, part, features)
    near_sum = block(near_out, x) + sum(fetch(block(near_out, (x - s) & 3), X, s) for s in (1, 2, 3))
    far_sum = block(far_out, y) + sum(fetch(block(far_out, (y - s) & 3), Y, s) for s in (1, 2, 3))
    both = jnp.where(zh == 0, jnp.stack([near_sum, far_sum]), jnp.stack([far_sum, near_sum]))

    tall, wide = part // 16, features // 256

    def tiled(value):
        return value.reshape(-1, 2, tall, 8, 2, wide, 128).transpose(0, 1, 4, 2, 5, 3, 6)

    pieces = tiled(both).reshape(8, -1, 128)
    near_loss = summed(own_sum, (Y, C))
    pieces = jnp.concatenate([pieces, jnp.broadcast_to(near_loss, (8, 8, 128))], axis=1)
    pieces = lax.all_to_all(pieces, (ZH, ZL), split_axis=0, concat_axis=0, tiled=True).sum(axis=0)
    piece = pieces[:-8]

    mine = tiled(block(w_key.reshape(4, part, features), x)).reshape(4, -1, 128)
    share = (piece * block(mine, lax.axis_index(ZL)).astype(jnp.float32)).sum(axis=1)
    share = jnp.concatenate([share, pieces[-1, :8]])
    lines = []
    for _ in range(3):
        lines.append(lax.reduce_precision(share, 8, 7))
        share = share - lines[-1]
    lines = jnp.pad(jnp.stack(lines), ((0, 5), (0, 0)))
    whole = from_everyone(jnp.concatenate([piece, lines]).astype(jnp.bfloat16), DP)
    shares = whole[:, -8:-5].astype(jnp.float32).sum(axis=1)
    loss = shares[:4, -1].sum() / (2.0 * features * total_count)
    shares = shares[:, :-8].reshape(2, 2, 4, tall, wide, 8)
    grad_gain = shares.sum(axis=(1, 4)).swapaxes(0, 1).reshape(own) / norm_gain.astype(jnp.float32)
    whole = whole[:, :-8].reshape(2, 2, 4, tall, wide, 8, 128)
    grad_key = whole.transpose(2, 0, 3, 5, 1, 4, 6).reshape(own, features).astype(jnp.float32)
    return (loss, grad_gain, grad_key)


def solution(mesh):
    split = Mesh(mesh.devices.reshape(4, 4, 2, 4, 2), DP_SHARD)
    return jax.shard_map(
        body,
        mesh=split,
        in_specs=(
            P(DP_SHARD, None),
            P(DP_SHARD, None),
            P(SHARD),
            P(SHARD, None),
            P(DP),
            P(DP, SHARD),
        ),
        out_specs=(P(), P(SHARD), P(SHARD, None)),
        check_vma=False,
    )
```

```python
import jax
import jax.numpy as jnp
from jax import lax
from jax.sharding import Mesh
from jax.sharding import PartitionSpec as P

ZL, X, ZH, Y, C = "dp_0", "dp_1", "shard_0", "shard_1", "shard_2"
SHARD = (ZH, Y, C)
DP_SHARD = (ZL, X, ZH, Y, C)
DP = (ZL, X)

EPSILON = 1e-06
SCALE = 1024.0


def fetch(value, axis, step):
    n = lax.axis_size(axis)
    return lax.ppermute(value, axis, [((i + step) % n, i) for i in range(n)])


def ring_blocks(value, axis, relay=True):
    one, three = (fetch(value, axis, step) for step in (1, 3))
    two = fetch(one, axis, 1) if relay else fetch(value, axis, 2)
    return [value, one, two, three]


def from_everyone(value, axes):
    copies = jnp.broadcast_to(value, (lax.axis_size(axes), *value.shape))
    return lax.all_to_all(copies, axes, split_axis=0, concat_axis=0, tiled=True)


def summed(value, axes):
    tile = jnp.broadcast_to(value, (8, 128))
    return from_everyone(tile, axes)[:, 0, 0].sum()


def block(value, *places):
    starts = [0 if at is None else at for at in places] + [0] * (value.ndim - len(places))
    sizes = [size if at is None else 1 for at, size in zip(places, value.shape)] + list(value.shape[len(places) :])
    kept = [size for at, size in zip(places, value.shape) if at is None] + list(value.shape[len(places) :])
    return lax.dynamic_slice(value, starts, sizes).reshape(kept)


def rows_by(left, right):
    return lax.dot_general(left, right, (((0,), (0,)), ((), ())), preferred_element_type=jnp.float32)


def body(hidden_in, teacher, norm_gain, w_key, group_rows, member):
    rows, width = hidden_in.shape
    own, features = w_key.shape
    part = own // 4
    x, y, zh, core = (lax.axis_index(name) for name in (X, Y, ZH, C))

    other = fetch(lax.dynamic_slice_in_dim(w_key, x * part, part), ZH, 1)
    near = ring_blocks(w_key, Y)
    quarter = jnp.zeros((4, part, features), w_key.dtype)
    for step, piece in enumerate(ring_blocks(other, Y, relay=False)):
        quarter = lax.dynamic_update_index_in_dim(quarter, piece, (y + step) & 3, 0)
    far = [block.reshape(own, features) for block in ring_blocks(quarter, X)]

    live_rows = group_rows[0]
    alive = member[0, 0]
    own_count = (alive * live_rows).astype(jnp.float32)
    gain_rows = jnp.pad(norm_gain.astype(jnp.float32), (0, 384 - own)).reshape(3, 128)
    tile = jnp.concatenate([gain_rows, jnp.broadcast_to(own_count, (5, 128))])
    tiles = from_everyone(tile, SHARD)
    gains = tiles[:, :3].reshape(-1, 384)[:, :own].reshape(width)
    total_count = summed(tiles[:, 3, 0].sum(), DP)

    values = hidden_in.astype(jnp.float32)
    inverse_rms = lax.rsqrt(jnp.mean(values * values, axis=1, keepdims=True) + EPSILON)
    normed = (values * inverse_rms * gains).astype(jnp.bfloat16)

    turned = normed.T.reshape(2, 4, 2, 4, part, rows)
    own_cols, their_cols = block(turned, None, None, core), block(turned, None, None, 1 - core)
    pair = jnp.concatenate([own_cols, fetch(their_cols, C, 1)], axis=-1)
    near_half = [block(pair, zh, (y + s) & 3).reshape(own, -1) for s in range(4)]
    far_half = [block(pair, 1 - zh, None, (x + s) & 3).reshape(own, -1) for s in range(4)]
    near_cols = [block(turned, zh, (y + s) & 3).reshape(2 * own, rows) for s in range(4)]
    far_cols = [block(turned, 1 - zh, None, None, (x + s) & 3).reshape(2 * own, rows) for s in range(4)]

    halves = rows_by(jnp.concatenate(near_half), jnp.concatenate(near)) + rows_by(far_half[0], far[0])
    halves += rows_by(jnp.concatenate([far_half[1], far_half[3]]), jnp.concatenate([far[1], far[3]]))
    halves += rows_by(far_half[2], far[2])
    keys = halves[:rows] + fetch(halves[rows:], C, 1)

    position = lax.broadcasted_iota(jnp.int32, (rows, 1), 0)
    valid = jnp.where((position < live_rows) & (alive == 1), 1.0, 0.0).astype(jnp.float32)
    diff = keys - teacher.astype(jnp.float32)
    own_sum = jnp.sum(valid * diff * diff)
    upstream = (SCALE / total_count * valid * diff).astype(jnp.bfloat16)

    near_in = [near_cols[0]] + [fetch(near_cols[4 - s], Y, s) for s in (1, 2, 3)]
    far_in = [far_cols[0]] + [fetch(far_cols[4 - s], X, s) for s in (1, 2, 3)]
    near_up = ring_blocks(upstream, Y)
    far_up = ring_blocks(upstream, X)

    def pooled(left, up, halve):
        first = jnp.dot(
            jnp.concatenate([left[i] for i in (0, 1, 3)], axis=1),
            jnp.concatenate([up[i] for i in (0, 1, 3)]),
            preferred_element_type=jnp.float32,
        )
        first = lax.optimization_barrier(first)
        sides = (1 - core, core)
        last = [halve(left[2], side) for side in sides]
        return [
            halve(first, side) + jnp.dot(half, up[2], preferred_element_type=jnp.float32)
            for side, half in zip(sides, last)
        ]

    def near_rows(value, side):
        return block(value.reshape(2, own, -1), side)

    def far_rows(value, side):
        return block(value.reshape(4, 2, part, -1), None, side).reshape(own, -1)

    near_other, near_mine = pooled(near_in, near_up, near_rows)
    far_other, far_mine = pooled(far_in, far_up, far_rows)
    near_out = (near_mine + fetch(near_other, C, 1)).reshape(4, part, features)
    far_out = (far_mine + fetch(far_other, C, 1)).reshape(4, part, features)
    near_sum = block(near_out, x) + sum(fetch(block(near_out, (x - s) & 3), X, s) for s in (1, 2, 3))
    far_sum = block(far_out, y) + sum(fetch(block(far_out, (y - s) & 3), Y, s) for s in (1, 2, 3))
    both = jnp.where(zh == 0, jnp.stack([near_sum, far_sum]), jnp.stack([far_sum, near_sum]))

    tall, wide = part // 16, features // 256

    def tiled(value):
        return value.reshape(-1, 2, tall, 8, 2, wide, 128).transpose(0, 1, 4, 2, 5, 3, 6)

    pieces = tiled(both).reshape(8, -1, 128)
    near_loss = summed(own_sum, (Y, C))
    pieces = jnp.concatenate([pieces, jnp.broadcast_to(near_loss, (8, 8, 128))], axis=1)
    pieces = lax.all_to_all(pieces, (ZH, ZL), split_axis=0, concat_axis=0, tiled=True).sum(axis=0)
    piece = pieces[:-8]

    mine = tiled(block(w_key.reshape(4, part, features), x)).reshape(4, -1, 128)
    share = (piece * block(mine, lax.axis_index(ZL)).astype(jnp.float32)).sum(axis=1)
    share = jnp.concatenate([share, pieces[-1, :8]])
    lines = []
    for _ in range(3):
        lines.append(lax.reduce_precision(share, 8, 7))
        share = share - lines[-1]
    lines = jnp.pad(jnp.stack(lines), ((0, 5), (0, 0)))
    whole = from_everyone(jnp.concatenate([piece, lines]).astype(jnp.bfloat16), DP)
    shares = whole[:, -8:-5].astype(jnp.float32).sum(axis=1)
    loss = shares[:4, -1].sum() / (2.0 * features * total_count)
    shares = shares[:, :-8].reshape(2, 2, 4, tall, wide, 8)
    grad_gain = shares.sum(axis=(1, 4)).swapaxes(0, 1).reshape(own) / norm_gain.astype(jnp.float32)
    whole = whole[:, :-8].reshape(2, 2, 4, tall, wide, 8, 128)
    grad_key = whole.transpose(2, 0, 3, 5, 1, 4, 6).reshape(own, features).astype(jnp.float32)
    return (loss, grad_gain, grad_key)


def solution(mesh):
    split = Mesh(mesh.devices.reshape(4, 4, 2, 4, 2), DP_SHARD)
    return jax.shard_map(
        body,
        mesh=split,
        in_specs=(
            P(DP_SHARD, None),
            P(DP_SHARD, None),
            P(SHARD),
            P(SHARD, None),
            P(DP),
            P(DP, SHARD),
        ),
        out_specs=(P(), P(SHARD), P(SHARD, None)),
        check_vma=False,
    )
```
